32 devices in a mesh: farcp: 4 (over x, core), nearcp: 2 (over y), heads: 4 (over z).
Axes of the slice: x: 2, y: 2, z: 4, core: 2. Of those that a mesh axis runs over, the one named last changes fastest.
Arguments:
- raw_keys: bfloat16 [8, 2048, 8, 128], P(None, ('farcp', 'nearcp'), 'heads'), may hold values from -6 to 6
- raw_values: bfloat16 [8, 2048, 8, 128], P(None, ('farcp', 'nearcp'), 'heads'), may hold values from -6 to 6
- turn_angle: float32 [2048, 64], replicated, may hold values from -3.140625 to 3.140625
- key_gain: float32 [128], replicated, may hold values from 0.25 to 1.75
Outputs:
- cache_keys: bfloat16 [8, 2048, 8, 128], P(('farcp', 'nearcp'), None, 'heads')
- cache_values: bfloat16 [8, 2048, 8, 128], P(('farcp', 'nearcp'), None, 'heads')
- key_scale: float32 [8, 8, 128], P(('farcp', 'nearcp'), 'heads')
The draws below stay inside these ranges and needn't reach their ends.
All inputs are finite; a program needn't handle non-finite values. Where the reference program divides by a largest or mean magnitude, that divisor is 1e-20 or more.
Results may differ from the reference program's by a relative error of at most 0.001.
Values may be sent and summed in bfloat16 or wider, within the bound.
No kernel may reach another device: no remote copies, remote signals or barrier semaphores. Data moves between devices by JAX's collectives and lax.ppermute only.
A program may use at most 128 MiB of HBM per device.

```python
import jax
import jax.numpy as jnp
from jax import lax

BATCH = 8
LENGTH = 2048
KV_HEADS = 8
HEAD_SIZE = 128
HALF_HEAD = 64


def block_scale(stream_key, dims, split, smallest, largest):
    gain = 1.0
    for position, blocks in split:
        heights = jax.random.uniform(jax.random.fold_in(jax.random.fold_in(stream_key, 6), position), (blocks,), jnp.float32, smallest / len(split), largest / len(split))
        gain = gain * jnp.repeat(jnp.exp(heights), dims[position] // blocks).reshape((-1,) + (1,) * (len(dims) - 1 - position))
    return gain


def normal_values(stream_key, shape, deviation, most, split=(), dtype=jnp.bfloat16):
    result = deviation * jax.random.normal(stream_key, shape, jnp.float32)
    if split:
        result = result * block_scale(stream_key, shape, split, -0.22, 0.18)
    return jnp.clip(result, -most, most).astype(dtype)


def setup_inputs(seed: int = 0) -> dict:
    streams_of = jax.random.split(jax.random.key(seed), 5)
    raw_keys = normal_values(streams_of[0], (BATCH, LENGTH, KV_HEADS, HEAD_SIZE), 1.0, 6.0, ((1, 8), (2, 4)))
    raw_values = normal_values(streams_of[1], (BATCH, LENGTH, KV_HEADS, HEAD_SIZE), 1.0, 6.0, ((1, 8), (2, 4)))
    turn_angle = jnp.clip(jax.random.uniform(streams_of[2], (LENGTH, HALF_HEAD), jnp.float32, -3.140625, 3.140625), -3.140625, 3.140625)
    key_gain = jnp.clip(1.0 + 0.15 * jax.random.normal(streams_of[3], (HEAD_SIZE,), jnp.float32), 0.25, 1.75)
    return dict(raw_keys=raw_keys, raw_values=raw_values, turn_angle=turn_angle, key_gain=key_gain)


def turn_pairs(vectors, angle):
    half = vectors.shape[-1] // 2
    cosine, sine = (jnp.cos(angle)[None, :, None, :], jnp.sin(angle)[None, :, None, :])
    first, second = (vectors[..., :half], vectors[..., half:])
    return jnp.concatenate([first * cosine - second * sine, second * cosine + first * sine], axis=-1)

def unit_rows(vectors, row_gain):
    return vectors * lax.rsqrt(lax.optimization_barrier(jnp.mean(vectors * vectors, axis=-1, keepdims=True)) + 1e-06) * row_gain

def ready_to_store(plain_keys, angle, key_gain):
    wide_keys = plain_keys.astype(jnp.float32)
    wide_keys = unit_rows(wide_keys, key_gain)
    return turn_pairs(wide_keys, angle)

def reference(raw_keys, raw_values, turn_angle, key_gain):
    turned_keys = ready_to_store(raw_keys, turn_angle, key_gain)
    key_scale = lax.optimization_barrier(jnp.max(jnp.abs(turned_keys), axis=1))
    narrow_keys = (turned_keys / key_scale[:, None]).astype(jnp.bfloat16)
    cache_keys = narrow_keys
    cache_values = raw_values
    return (cache_keys, cache_values, key_scale)
```

```python
import jax
import jax.numpy as jnp
from jax import lax
from jax.experimental import pallas as pl
from jax.experimental.pallas import tpu as pltpu
from jax.sharding import PartitionSpec as P

GROUP = ("farcp", "nearcp")


def turn_tables(angle, heads):
    cosine, sine = lax.optimization_barrier((jnp.cos(angle), jnp.sin(angle)))
    length, half = angle.shape
    rows = (length, heads, 2 * half)
    both = jnp.concatenate([cosine, cosine], axis=-1)[:, None, :]
    signed = jnp.concatenate([-sine, sine], axis=-1)[:, None, :]
    return (
        jnp.broadcast_to(both, rows).reshape(length * heads, 2 * half),
        jnp.broadcast_to(signed, rows).reshape(length * heads, 2 * half),
    )


def key_kernel(heads, keys_ref, cos_ref, sin_ref, gain_ref, narrow_ref, scale_ref, turned_ref):
    rows, size = turned_ref.shape
    step = 64 if rows % 64 == 0 else rows
    gain = gain_ref[...]
    group = 8 if (step % 8 == 0 and 8 % heads == 0) else heads

    def turn(i, most):
        at = pl.ds(i * step, step)
        wide = keys_ref[0, at, :].astype(jnp.float32)
        square = jnp.mean(wide * wide, axis=-1, keepdims=True)
        wide = wide * lax.rsqrt(square + 1e-06) * gain
        turned = wide * cos_ref[at, :] + pltpu.roll(wide, size // 2, 1) * sin_ref[at, :]
        turned_ref[at, :] = turned
        return jnp.maximum(most, jnp.max(jnp.abs(turned).reshape(step // group, group, size), axis=0))

    most = lax.fori_loop(0, rows // step, turn, jnp.zeros((group, size), jnp.float32))
    peaks = [
        jnp.max(jnp.concatenate([most[g : g + 1] for g in range(h, group, heads)], axis=0), axis=0, keepdims=True)
        for h in range(heads)
    ]
    scale = jnp.concatenate(peaks, axis=0)
    scale_ref[0] = scale
    inverse = 1.0 / jnp.concatenate([scale] * (group // heads), axis=0)

    def narrow(i, carry):
        at = pl.ds(i * step, step)
        turned = turned_ref[at, :].reshape(step // group, group, size)
        narrow_ref[0, at, :] = (turned * inverse[None]).reshape(step, size).astype(jnp.bfloat16)
        return carry

    lax.fori_loop(0, rows // step, narrow, 0)


def ready_keys(moved_keys, angle, key_gain):
    batch, length, heads, size = moved_keys.shape
    rows = length * heads
    cosine, sine = turn_tables(angle, heads)
    whole = lambda b: (0, 0)
    narrow, scale = pl.pallas_call(
        lambda *refs: key_kernel(heads, *refs),
        grid=(batch,),
        in_specs=[
            pl.BlockSpec((1, rows, size), lambda b: (b, 0, 0)),
            pl.BlockSpec((rows, size), whole),
            pl.BlockSpec((rows, size), whole),
            pl.BlockSpec((1, size), whole),
        ],
        out_specs=[
            pl.BlockSpec((1, rows, size), lambda b: (b, 0, 0)),
            pl.BlockSpec((1, heads, size), lambda b: (b, 0, 0)),
        ],
        out_shape=[
            jax.ShapeDtypeStruct((batch, rows, size), jnp.bfloat16),
            jax.ShapeDtypeStruct((batch, heads, size), jnp.float32),
        ],
        scratch_shapes=[pltpu.VMEM((rows, size), jnp.float32)],
        compiler_params=pltpu.CompilerParams(vmem_limit_bytes=48 * 1024 * 1024),
    )(moved_keys.reshape(batch, rows, size), cosine, sine, key_gain[None])
    return narrow.reshape(batch, length, heads, size), scale


def to_sequences(spread):
    batch, length, heads, size = spread.shape
    members = lax.axis_size(GROUP)
    moved = lax.all_to_all(spread, GROUP, split_axis=0, concat_axis=0, tiled=True)
    if batch != members:
        moved = jnp.swapaxes(moved.reshape(members, batch // members, length, heads, size), 0, 1)
    return moved.reshape(batch // members, length * members, heads, size)


def shards(raw_keys, raw_values, turn_angle, key_gain):
    moved_keys = to_sequences(raw_keys)
    cache_values = to_sequences(raw_values)
    narrow_keys, key_scale = ready_keys(moved_keys, turn_angle, key_gain)
    return (narrow_keys, cache_values, key_scale)


def solution(mesh):
    in_specs = (
        P(None, GROUP, "heads", None),
        P(None, GROUP, "heads", None),
        P(),
        P(),
    )
    out_specs = (
        P(GROUP, None, "heads", None),
        P(GROUP, None, "heads", None),
        P(GROUP, "heads", None),
    )
    return jax.shard_map(shards, mesh=mesh, in_specs=in_specs, out_specs=out_specs, check_vma=False)
```

```python
import jax
import jax.numpy as jnp
from jax import lax
from jax.experimental import pallas as pl
from jax.experimental.pallas import tpu as pltpu
from jax.sharding import PartitionSpec as P

GROUP = ("farcp", "nearcp")


def turn_tables(angle, heads):
    cosine, sine = lax.optimization_barrier((jnp.cos(angle), jnp.sin(angle)))
    length, half = angle.shape
    rows = (length, heads, 2 * half)
    both = jnp.concatenate([cosine, cosine], axis=-1)[:, None, :]
    signed = jnp.concatenate([-sine, sine], axis=-1)[:, None, :]
    return (
        jnp.broadcast_to(both, rows).reshape(length * heads, 2 * half),
        jnp.broadcast_to(signed, rows).reshape(length * heads, 2 * half),
    )


def peer_of(rank, hop, members):
    if members & (members - 1) == 0:
        return rank ^ hop, rank ^ hop
    return (rank + hop) % members, (rank - hop) % members


def exchange(spread):
    batch = spread.shape[0]
    members = lax.axis_size(GROUP)
    rank = lax.axis_index(GROUP)
    share = batch // members
    pieces = [lax.dynamic_slice_in_dim(spread, rank * share, share, axis=0)]
    for hop in range(1, members):
        target = peer_of(rank, hop, members)[0]
        block = lax.dynamic_slice_in_dim(spread, target * share, share, axis=0)
        route = [(r, peer_of(r, hop, members)[0]) for r in range(members)]
        pieces.append(lax.ppermute(block, GROUP, route))
    return pieces


def sources():
    members = lax.axis_size(GROUP)
    rank = lax.axis_index(GROUP)
    return jnp.stack([peer_of(rank, hop, members)[1] for hop in range(members)]).astype(jnp.int32)


def key_kernel(heads, members, from_ref, *refs):
    pieces, (cos_ref, sin_ref, gain_ref, narrow_ref, scale_ref, turned_ref) = refs[:members], refs[members:]
    rows, size = turned_ref.shape
    part = rows // members
    step = 256 if part % 256 == 0 else part
    gain = gain_ref[...]
    group = 8 if (step % 8 == 0 and 8 % heads == 0) else heads
    most = jnp.zeros((group, size), jnp.float32)

    for hop in range(members):
        base = from_ref[hop] * part
        for i in range(part // step):
            at = pl.ds(pl.multiple_of(base + i * step, step), step)
            wide = pieces[hop][0, i * step : (i + 1) * step, :].astype(jnp.float32)
            square = jnp.mean(wide * wide, axis=-1, keepdims=True)
            wide = wide * lax.rsqrt(square + 1e-06) * gain
            turned = wide * cos_ref[at, :] + pltpu.roll(wide, size // 2, 1) * sin_ref[at, :]
            turned_ref[at, :] = turned
            most = jnp.maximum(most, jnp.max(jnp.abs(turned).reshape(step // group, group, size), axis=0))

    peaks = [
        jnp.max(jnp.concatenate([most[g : g + 1] for g in range(h, group, heads)], axis=0), axis=0, keepdims=True)
        for h in range(heads)
    ]
    scale = jnp.concatenate(peaks, axis=0)
    scale_ref[0] = scale
    inverse = 1.0 / jnp.concatenate([scale] * (group // heads), axis=0)

    def narrow(i, carry):
        at = pl.ds(pl.multiple_of(i * step, step), step)
        turned = turned_ref[at, :].reshape(step // group, group, size)
        narrow_ref[0, at, :] = (turned * inverse[None]).reshape(step, size).astype(jnp.bfloat16)
        return carry

    lax.fori_loop(0, rows // step, narrow, 0)


def ready_keys(pieces, order, angle, key_gain):
    members = len(pieces)
    batch, length, heads, size = pieces[0].shape
    part = length * heads
    rows = members * part
    cosine, sine = turn_tables(angle, heads)
    whole = lambda b, order: (0, 0)
    piece = pl.BlockSpec((1, part, size), lambda b, order: (b, 0, 0))
    narrow, scale = pl.pallas_call(
        lambda *refs: key_kernel(heads, members, *refs),
        grid_spec=pltpu.PrefetchScalarGridSpec(
            num_scalar_prefetch=1,
            grid=(batch,),
            in_specs=[piece] * members
            + [pl.BlockSpec((rows, size), whole), pl.BlockSpec((rows, size), whole), pl.BlockSpec((1, size), whole)],
            out_specs=[
                pl.BlockSpec((1, rows, size), lambda b, order: (b, 0, 0)),
                pl.BlockSpec((1, heads, size), lambda b, order: (b, 0, 0)),
            ],
            scratch_shapes=[pltpu.VMEM((rows, size), jnp.float32)],
        ),
        out_shape=[
            jax.ShapeDtypeStruct((batch, rows, size), jnp.bfloat16),
            jax.ShapeDtypeStruct((batch, heads, size), jnp.float32),
        ],
        compiler_params=pltpu.CompilerParams(vmem_limit_bytes=48 * 1024 * 1024),
    )(order, *[p.reshape(batch, part, size) for p in pieces], cosine, sine, key_gain[None])
    return narrow.reshape(batch, rows // heads, heads, size), scale


def place_kernel(members, from_ref, *refs):
    pieces, (out_ref, sems) = refs[:members], refs[members:]
    part = pieces[0].shape[1]
    copies = [
        pltpu.make_async_copy(pieces[hop], out_ref.at[:, pl.ds(from_ref[hop] * part, part)], sems.at[hop])
        for hop in range(members)
    ]
    for copy in copies:
        copy.start()
    for copy in copies:
        copy.wait()


def place(pieces, order):
    members = len(pieces)
    batch, length, heads, size = pieces[0].shape
    anywhere = pl.BlockSpec(memory_space=pl.ANY)
    return pl.pallas_call(
        lambda *refs: place_kernel(members, *refs),
        grid_spec=pltpu.PrefetchScalarGridSpec(
            num_scalar_prefetch=1,
            grid=(1,),
            in_specs=[anywhere] * members,
            out_specs=anywhere,
            scratch_shapes=[pltpu.SemaphoreType.DMA((members,))],
        ),
        out_shape=jax.ShapeDtypeStruct((batch, members * length, heads, size), pieces[0].dtype),
    )(order, *pieces)


def shards(raw_keys, raw_values, turn_angle, key_gain):
    order = sources()
    key_pieces = exchange(raw_keys)
    value_pieces = exchange(raw_values)
    narrow_keys, key_scale = ready_keys(key_pieces, order, turn_angle, key_gain)
    return (narrow_keys, place(value_pieces, order), key_scale)


def solution(mesh):
    in_specs = (
        P(None, GROUP, "heads", None),
        P(None, GROUP, "heads", None),
        P(),
        P(),
    )
    out_specs = (
        P(GROUP, None, "heads", None),
        P(GROUP, None, "heads", None),
        P(GROUP, "heads", None),
    )
    return jax.shard_map(shards, mesh=mesh, in_specs=in_specs, out_specs=out_specs, check_vma=False)
```

```python
import jax
import jax.numpy as jnp
from jax import lax
from jax.experimental import pallas as pl
from jax.experimental.pallas import tpu as pltpu
from jax.sharding import PartitionSpec as P

GROUP = ("farcp", "nearcp")


def turn_tables(angle, heads):
    cosine, sine = lax.optimization_barrier((jnp.cos(angle), jnp.sin(angle)))
    length, half = angle.shape
    rows = (length, heads, 2 * half)
    both = jnp.concatenate([cosine, cosine], axis=-1)[:, None, :]
    signed = jnp.concatenate([-sine, sine], axis=-1)[:, None, :]
    return (
        jnp.broadcast_to(both, rows).reshape(length * heads, 2 * half),
        jnp.broadcast_to(signed, rows).reshape(length * heads, 2 * half),
    )


def peer_of(rank, hop, members):
    if members & (members - 1) == 0:
        return rank ^ hop, rank ^ hop
    return (rank + hop) % members, (rank - hop) % members


def hops_of(members):
    far = list(range(members - 1, members // 2 - 1, -1))
    near = list(range(1, members // 2, 2)) + list(range(2, members // 2, 2))
    hops = [0]
    while far or near:
        hops += far[:1] + near[:1]
        far, near = far[1:], near[1:]
    return hops


def exchange(spread):
    batch = spread.shape[0]
    members = lax.axis_size(GROUP)
    rank = lax.axis_index(GROUP)
    share = batch // members
    pieces = [lax.dynamic_slice_in_dim(spread, rank * share, share, axis=0)]
    for hop in hops_of(members)[1:]:
        target = peer_of(rank, hop, members)[0]
        block = lax.dynamic_slice_in_dim(spread, target * share, share, axis=0)
        route = [(r, peer_of(r, hop, members)[0]) for r in range(members)]
        pieces.append(lax.ppermute(block, GROUP, route))
    return pieces


def sources():
    members = lax.axis_size(GROUP)
    rank = lax.axis_index(GROUP)
    return jnp.stack([peer_of(rank, hop, members)[1] for hop in hops_of(members)]).astype(jnp.int32)


def key_kernel(heads, members, from_ref, *refs):
    pieces, (cos_ref, sin_ref, gain_ref, narrow_ref, scale_ref, turned_ref) = refs[:members], refs[members:]
    rows, size = turned_ref.shape
    part = rows // members
    step = 256 if part % 256 == 0 else part
    gain = gain_ref[...]
    group = 8 if (step % 8 == 0 and 8 % heads == 0) else heads
    most = jnp.zeros((group, size), jnp.float32)

    for hop in range(members):
        base = from_ref[hop] * part
        for i in range(part // step):
            at = pl.ds(pl.multiple_of(base + i * step, step), step)
            wide = pieces[hop][0, i * step : (i + 1) * step, :].astype(jnp.float32)
            square = jnp.mean(wide * wide, axis=-1, keepdims=True)
            wide = wide * lax.rsqrt(square + 1e-06) * gain
            turned = wide * cos_ref[at, :] + pltpu.roll(wide, size // 2, 1) * sin_ref[at, :]
            turned_ref[at, :] = turned
            most = jnp.maximum(most, jnp.max(jnp.abs(turned).reshape(step // group, group, size), axis=0))

    peaks = [
        jnp.max(jnp.concatenate([most[g : g + 1] for g in range(h, group, heads)], axis=0), axis=0, keepdims=True)
        for h in range(heads)
    ]
    scale = jnp.concatenate(peaks, axis=0)
    scale_ref[0] = scale
    inverse = 1.0 / jnp.concatenate([scale] * (group // heads), axis=0)

    def narrow(i, carry):
        at = pl.ds(pl.multiple_of(i * step, step), step)
        turned = turned_ref[at, :].reshape(step // group, group, size)
        narrow_ref[0, at, :] = (turned * inverse[None]).reshape(step, size).astype(jnp.bfloat16)
        return carry

    lax.fori_loop(0, rows // step, narrow, 0)


def ready_keys(pieces, order, angle, key_gain):
    members = len(pieces)
    batch, length, heads, size = pieces[0].shape
    part = length * heads
    rows = members * part
    cosine, sine = turn_tables(angle, heads)
    whole = lambda b, order: (0, 0)
    piece = pl.BlockSpec((1, part, size), lambda b, order: (b, 0, 0))
    narrow, scale = pl.pallas_call(
        lambda *refs: key_kernel(heads, members, *refs),
        grid_spec=pltpu.PrefetchScalarGridSpec(
            num_scalar_prefetch=1,
            grid=(batch,),
            in_specs=[piece] * members
            + [pl.BlockSpec((rows, size), whole), pl.BlockSpec((rows, size), whole), pl.BlockSpec((1, size), whole)],
            out_specs=[
                pl.BlockSpec((1, rows, size), lambda b, order: (b, 0, 0)),
                pl.BlockSpec((1, heads, size), lambda b, order: (b, 0, 0)),
            ],
            scratch_shapes=[pltpu.VMEM((rows, size), jnp.float32)],
        ),
        out_shape=[
            jax.ShapeDtypeStruct((batch, rows, size), jnp.bfloat16),
            jax.ShapeDtypeStruct((batch, heads, size), jnp.float32),
        ],
        compiler_params=pltpu.CompilerParams(vmem_limit_bytes=48 * 1024 * 1024),
    )(order, *[p.reshape(batch, part, size) for p in pieces], cosine, sine, key_gain[None])
    return narrow.reshape(batch, rows // heads, heads, size), scale


def place_kernel(members, from_ref, *refs):
    pieces, (out_ref, sems) = refs[:members], refs[members:]
    part = pieces[0].shape[1]
    copies = [
        pltpu.make_async_copy(pieces[hop], out_ref.at[:, pl.ds(pl.multiple_of(from_ref[hop] * part, part), part)], sems.at[hop])
        for hop in range(members)
    ]
    for copy in copies:
        copy.start()
    for copy in copies:
        copy.wait()


def place(pieces, order):
    members = len(pieces)
    batch, length, heads, size = pieces[0].shape
    part = length * heads
    anywhere = pl.BlockSpec(memory_space=pl.ANY)
    return pl.pallas_call(
        lambda *refs: place_kernel(members, *refs),
        grid_spec=pltpu.PrefetchScalarGridSpec(
            num_scalar_prefetch=1,
            grid=(1,),
            in_specs=[anywhere] * members,
            out_specs=anywhere,
            scratch_shapes=[pltpu.SemaphoreType.DMA((members,))],
        ),
        out_shape=jax.ShapeDtypeStruct((batch, members * part, size), pieces[0].dtype),
    )(order, *[p.reshape(batch, part, size) for p in pieces]).reshape(batch, members * length, heads, size)


def shards(raw_keys, raw_values, turn_angle, key_gain):
    order = sources()
    key_pieces = exchange(raw_keys)
    value_pieces = exchange(raw_values)
    narrow_keys, key_scale = ready_keys(key_pieces, order, turn_angle, key_gain)
    return (narrow_keys, place(value_pieces, order), key_scale)


def solution(mesh):
    in_specs = (
        P(None, GROUP, "heads", None),
        P(None, GROUP, "heads", None),
        P(),
        P(),
    )
    out_specs = (
        P(GROUP, None, "heads", None),
        P(GROUP, None, "heads", None),
        P(GROUP, "heads", None),
    )
    return jax.shard_map(shards, mesh=mesh, in_specs=in_specs, out_specs=out_specs, check_vma=False)
```

```python
import jax
import jax.numpy as jnp
from jax import lax
from jax.experimental import pallas as pl
from jax.experimental.pallas import tpu as pltpu
from jax.sharding import PartitionSpec as P

GROUP = ("farcp", "nearcp")


def turn_tables(angle, heads):
    cosine, sine = lax.optimization_barrier((jnp.cos(angle), jnp.sin(angle)))
    length, half = angle.shape
    rows = (length, heads, 2 * half)
    both = jnp.concatenate([cosine, cosine], axis=-1)[:, None, :]
    signed = jnp.concatenate([-sine, sine], axis=-1)[:, None, :]
    return (
        jnp.broadcast_to(both, rows).reshape(length * heads, 2 * half),
        jnp.broadcast_to(signed, rows).reshape(length * heads, 2 * half),
    )


def peer_of(rank, hop, members):
    if members & (members - 1) == 0:
        return rank ^ hop, rank ^ hop
    return (rank + hop) % members, (rank - hop) % members


def hops_of(members):
    far = list(range(members - 1, members // 2 - 1, -1))
    near = list(range(1, members // 2, 2)) + list(range(2, members // 2, 2))
    hops = [0]
    while far or near:
        hops += far[:1] + near[:1]
        far, near = far[1:], near[1:]
    return hops


def exchange(spread):
    batch = spread.shape[0]
    members = lax.axis_size(GROUP)
    rank = lax.axis_index(GROUP)
    share = batch // members
    pieces = [lax.dynamic_slice_in_dim(spread, rank * share, share, axis=0)]
    for hop in hops_of(members)[1:]:
        target = peer_of(rank, hop, members)[0]
        block = lax.dynamic_slice_in_dim(spread, target * share, share, axis=0)
        route = [(r, peer_of(r, hop, members)[0]) for r in range(members)]
        pieces.append(lax.ppermute(block, GROUP, route))
    return pieces


def sources():
    members = lax.axis_size(GROUP)
    rank = lax.axis_index(GROUP)
    return jnp.stack([peer_of(rank, hop, members)[1] for hop in hops_of(members)]).astype(jnp.int32)


def key_kernel(heads, members, from_ref, *refs):
    pieces, (cos_ref, sin_ref, gain_ref, narrow_ref, scale_ref, turned_ref) = refs[:members], refs[members:]
    rows, size = turned_ref.shape
    part = rows // members
    step = 256 if part % 256 == 0 else part
    gain = gain_ref[...]
    group = 8 if (step % 8 == 0 and 8 % heads == 0) else heads
    most = jnp.zeros((group, size), jnp.float32)

    for hop in range(members):
        base = from_ref[hop] * part
        for i in range(part // step):
            at = pl.ds(pl.multiple_of(base + i * step, step), step)
            wide = pieces[hop][0, i * step : (i + 1) * step, :].astype(jnp.float32)
            square = jnp.mean(wide * wide, axis=-1, keepdims=True)
            wide = wide * lax.rsqrt(square + 1e-06) * gain
            turned = wide * cos_ref[at, :] + pltpu.roll(wide, size // 2, 1) * sin_ref[at, :]
            turned_ref[at, :] = turned
            most = jnp.maximum(most, jnp.max(jnp.abs(turned).reshape(step // group, group, size), axis=0))

    peaks = [
        jnp.max(jnp.concatenate([most[g : g + 1] for g in range(h, group, heads)], axis=0), axis=0, keepdims=True)
        for h in range(heads)
    ]
    scale = jnp.concatenate(peaks, axis=0)
    scale_ref[0] = scale
    inverse = 1.0 / jnp.concatenate([scale] * (group // heads), axis=0)

    def narrow(i, carry):
        at = pl.ds(pl.multiple_of(i * step, step), step)
        turned = turned_ref[at, :].reshape(step // group, group, size)
        narrow_ref[0, at, :] = (turned * inverse[None]).reshape(step, size).astype(jnp.bfloat16)
        return carry

    lax.fori_loop(0, rows // step, narrow, 0)


def ready_keys(pieces, order, angle, key_gain):
    members = len(pieces)
    batch, length, heads, size = pieces[0].shape
    part = length * heads
    rows = members * part
    cosine, sine = turn_tables(angle, heads)
    whole = lambda b, order: (0, 0)
    piece = pl.BlockSpec((1, part, size), lambda b, order: (b, 0, 0))
    narrow, scale = pl.pallas_call(
        lambda *refs: key_kernel(heads, members, *refs),
        grid_spec=pltpu.PrefetchScalarGridSpec(
            num_scalar_prefetch=1,
            grid=(batch,),
            in_specs=[piece] * members
            + [pl.BlockSpec((rows, size), whole), pl.BlockSpec((rows, size), whole), pl.BlockSpec((1, size), whole)],
            out_specs=[
                pl.BlockSpec((1, rows, size), lambda b, order: (b, 0, 0)),
                pl.BlockSpec((1, heads, size), lambda b, order: (b, 0, 0)),
            ],
            scratch_shapes=[pltpu.VMEM((rows, size), jnp.float32)],
        ),
        out_shape=[
            jax.ShapeDtypeStruct((batch, rows, size), jnp.bfloat16),
            jax.ShapeDtypeStruct((batch, heads, size), jnp.float32),
        ],
        compiler_params=pltpu.CompilerParams(vmem_limit_bytes=48 * 1024 * 1024),
    )(order, *[p.reshape(batch, part, size) for p in pieces], cosine, sine, key_gain[None])
    return narrow.reshape(batch, rows // heads, heads, size), scale


def place_kernel(members, from_ref, *refs):
    pieces, (out_ref, sems) = refs[:members], refs[members:]
    part = pieces[0].shape[1]
    copies = [
        pltpu.make_async_copy(pieces[hop], out_ref.at[:, pl.ds(pl.multiple_of(from_ref[hop] * part, part), part)], sems.at[hop])
        for hop in range(members)
    ]
    for copy in copies:
        copy.start()
    for copy in copies:
        copy.wait()


def place(pieces, order):
    members = len(pieces)
    batch, length, heads, size = pieces[0].shape
    part = length * heads
    anywhere = pl.BlockSpec(memory_space=pl.ANY)
    return pl.pallas_call(
        lambda *refs: place_kernel(members, *refs),
        grid_spec=pltpu.PrefetchScalarGridSpec(
            num_scalar_prefetch=1,
            grid=(1,),
            in_specs=[pl.BlockSpec((batch, part, size), lambda i, order: (0, 0, 0))] * members,
            out_specs=anywhere,
            scratch_shapes=[pltpu.SemaphoreType.DMA((members,))],
        ),
        out_shape=jax.ShapeDtypeStruct((batch, members * part, size), pieces[0].dtype),
    )(order, *[p.reshape(batch, part, size) for p in pieces]).reshape(batch, members * length, heads, size)


def shards(raw_keys, raw_values, turn_angle, key_gain):
    order = sources()
    key_pieces = exchange(raw_keys)
    value_pieces = exchange(raw_values)
    narrow_keys, key_scale = ready_keys(key_pieces, order, turn_angle, key_gain)
    late_order, key_scale = lax.optimization_barrier((order, key_scale))
    return (narrow_keys, place(value_pieces, late_order), key_scale)


def solution(mesh):
    in_specs = (
        P(None, GROUP, "heads", None),
        P(None, GROUP, "heads", None),
        P(),
        P(),
    )
    out_specs = (
        P(GROUP, None, "heads", None),
        P(GROUP, None, "heads", None),
        P(GROUP, "heads", None),
    )
    return jax.shard_map(shards, mesh=mesh, in_specs=in_specs, out_specs=out_specs, check_vma=False)
```

```python
import jax
import jax.numpy as jnp
from jax import lax
from jax.experimental import pallas as pl
from jax.experimental.pallas import tpu as pltpu
from jax.sharding import PartitionSpec as P

GROUP = ("farcp", "nearcp")


def turn_tables(angle):
    cosine, sine = lax.optimization_barrier((jnp.cos(angle), jnp.sin(angle)))
    return jnp.concatenate([cosine, cosine], axis=-1), jnp.concatenate([-sine, sine], axis=-1)


def peer_of(rank, hop, members):
    if members & (members - 1) == 0:
        return rank ^ hop, rank ^ hop
    return (rank + hop) % members, (rank - hop) % members


def hops_of(members):
    far = list(range(members - 1, members // 2 - 1, -1))
    near = list(range(1, members // 2, 2)) + list(range(2, members // 2, 2))
    hops = [0]
    while far or near:
        hops += far[:1] + near[:1]
        far, near = far[1:], near[1:]
    return hops


def exchange(spread):
    batch = spread.shape[0]
    members = lax.axis_size(GROUP)
    rank = lax.axis_index(GROUP)
    share = batch // members
    pieces = [lax.dynamic_slice_in_dim(spread, rank * share, share, axis=0)]
    for hop in hops_of(members)[1:]:
        target = peer_of(rank, hop, members)[0]
        block = lax.dynamic_slice_in_dim(spread, target * share, share, axis=0)
        route = [(r, peer_of(r, hop, members)[0]) for r in range(members)]
        pieces.append(lax.ppermute(block, GROUP, route))
    return pieces


def sources():
    members = lax.axis_size(GROUP)
    rank = lax.axis_index(GROUP)
    return jnp.stack([peer_of(rank, hop, members)[1] for hop in hops_of(members)]).astype(jnp.int32)


def key_kernel(heads, members, from_ref, *refs):
    pieces, (cos_ref, sin_ref, gain_ref, narrow_ref, scale_ref, turned_ref) = refs[:members], refs[members:]
    rows, size = turned_ref.shape
    part = rows // members
    step = 256 if part % 256 == 0 else part
    gain = gain_ref[...]
    group = 8 if (step % 8 == 0 and 8 % heads == 0) else heads
    most = jnp.zeros((group, size), jnp.float32)

    for hop in range(members):
        base = from_ref[hop] * part
        for i in range(part // step):
            at = pl.ds(pl.multiple_of(base + i * step, step), step)
            wide = pieces[hop][0, i * step : (i + 1) * step, :].astype(jnp.float32)
            square = jnp.mean(wide * wide, axis=-1, keepdims=True)
            wide = wide * lax.rsqrt(square + 1e-06) * gain
            spots = pl.ds(pl.multiple_of((base + i * step) // heads, step // heads), step // heads)
            spread = (step // heads, heads, size)
            cosine = jnp.broadcast_to(cos_ref[spots, :][:, None, :], spread).reshape(step, size)
            sine = jnp.broadcast_to(sin_ref[spots, :][:, None, :], spread).reshape(step, size)
            turned = wide * cosine + pltpu.roll(wide, size // 2, 1) * sine
            turned_ref[at, :] = turned
            most = jnp.maximum(most, jnp.max(jnp.abs(turned).reshape(step // group, group, size), axis=0))

    peaks = [
        jnp.max(jnp.concatenate([most[g : g + 1] for g in range(h, group, heads)], axis=0), axis=0, keepdims=True)
        for h in range(heads)
    ]
    scale = jnp.concatenate(peaks, axis=0)
    scale_ref[0] = scale
    inverse = 1.0 / jnp.concatenate([scale] * (group // heads), axis=0)

    def narrow(i, carry):
        at = pl.ds(pl.multiple_of(i * step, step), step)
        turned = turned_ref[at, :].reshape(step // group, group, size)
        narrow_ref[0, at, :] = (turned * inverse[None]).reshape(step, size).astype(jnp.bfloat16)
        return carry

    lax.fori_loop(0, rows // step, narrow, 0)


def ready_keys(pieces, order, angle, key_gain):
    members = len(pieces)
    batch, length, heads, size = pieces[0].shape
    part = length * heads
    rows = members * part
    cosine, sine = turn_tables(angle)
    whole = lambda b, order: (0, 0)
    piece = pl.BlockSpec((1, part, size), lambda b, order: (b, 0, 0))
    narrow, scale = pl.pallas_call(
        lambda *refs: key_kernel(heads, members, *refs),
        grid_spec=pltpu.PrefetchScalarGridSpec(
            num_scalar_prefetch=1,
            grid=(batch,),
            in_specs=[piece] * members
            + [pl.BlockSpec((rows // heads, size), whole)] * 2 + [pl.BlockSpec((1, size), whole)],
            out_specs=[
                pl.BlockSpec((1, rows, size), lambda b, order: (b, 0, 0)),
                pl.BlockSpec((1, heads, size), lambda b, order: (b, 0, 0)),
            ],
            scratch_shapes=[pltpu.VMEM((rows, size), jnp.float32)],
        ),
        out_shape=[
            jax.ShapeDtypeStruct((batch, rows, size), jnp.bfloat16),
            jax.ShapeDtypeStruct((batch, heads, size), jnp.float32),
        ],
        compiler_params=pltpu.CompilerParams(vmem_limit_bytes=48 * 1024 * 1024),
    )(order, *[p.reshape(batch, part, size) for p in pieces], cosine, sine, key_gain[None])
    return narrow.reshape(batch, rows // heads, heads, size), scale


def place_kernel(members, from_ref, *refs):
    pieces, (out_ref, sems) = refs[:members], refs[members:]
    part = pieces[0].shape[1]
    copies = [
        pltpu.make_async_copy(pieces[hop], out_ref.at[:, pl.ds(pl.multiple_of(from_ref[hop] * part, part), part)], sems.at[hop])
        for hop in range(members)
    ]
    for copy in copies:
        copy.start()
    for copy in copies:
        copy.wait()


def place(pieces, order):
    members = len(pieces)
    batch, length, heads, size = pieces[0].shape
    part = length * heads
    anywhere = pl.BlockSpec(memory_space=pl.ANY)
    return pl.pallas_call(
        lambda *refs: place_kernel(members, *refs),
        grid_spec=pltpu.PrefetchScalarGridSpec(
            num_scalar_prefetch=1,
            grid=(1,),
            in_specs=[pl.BlockSpec((batch, part, size), lambda i, order: (0, 0, 0))] * members,
            out_specs=anywhere,
            scratch_shapes=[pltpu.SemaphoreType.DMA((members,))],
        ),
        out_shape=jax.ShapeDtypeStruct((batch, members * part, size), pieces[0].dtype),
    )(order, *[p.reshape(batch, part, size) for p in pieces]).reshape(batch, members * length, heads, size)


def shards(raw_keys, raw_values, turn_angle, key_gain):
    order = sources()
    key_pieces = exchange(raw_keys)
    value_pieces = exchange(raw_values)
    narrow_keys, key_scale = ready_keys(key_pieces, order, turn_angle, key_gain)
    late_order, key_scale = lax.optimization_barrier((order, key_scale))
    return (narrow_keys, place(value_pieces, late_order), key_scale)


def solution(mesh):
    in_specs = (
        P(None, GROUP, "heads", None),
        P(None, GROUP, "heads", None),
        P(),
        P(),
    )
    out_specs = (
        P(GROUP, None, "heads", None),
        P(GROUP, None, "heads", None),
        P(GROUP, "heads", None),
    )
    return jax.shard_map(shards, mesh=mesh, in_specs=in_specs, out_specs=out_specs, check_vma=False)
```
